256 devices in a mesh: rep: 32 (over z, y), data: 8 (over x, core).
Axes of the slice: x: 4, y: 4, z: 8, core: 2. Of those that a mesh axis runs over, the one named last changes fastest.
Arguments:
- w1: bfloat16 [2, 1536, 6144], replicated
- w2: bfloat16 [2, 6144, 1536], replicated
- x: bfloat16 [768, 1, 64, 1536], P(('rep', 'data'))
- dy: bfloat16 [768, 1, 64, 1536], P(('rep', 'data'))
Outputs:
- output 1: bfloat16 [2, 1536, 6144], replicated
- output 2: bfloat16 [2, 6144, 1536], replicated
- output 3: bfloat16 [768, 1, 64, 1536], P(('rep', 'data'))
All inputs are finite; a program needn't handle non-finite values.
Results may differ from the reference program's by a relative error of at most 0.02.
Values are sent between devices in bfloat16 or wider.
A program may use at most 768 MiB of HBM per device.

```python
import jax
import jax.numpy as jnp
from jax import lax

D = 1536
FF = 6144
LAYERS = 2
MICRO = 3
BATCH = 1
SEQ = 64
NDEV = 256

GC = 0.7978845608028654
GA = 0.044715


def gelu_pair(u):
    t = jnp.tanh(GC * (u + GA * u * u * u))
    val = 0.5 * u * (1.0 + t)
    der = 0.5 * (1.0 + t) + 0.5 * u * (1.0 - t * t) * GC * (1.0 + 3.0 * GA * u * u)
    return val, der


def setup_inputs(seed: int = 0) -> dict:
    key = jax.random.key(seed)
    k1, k2, k3, k4 = jax.random.split(key, 4)
    rows = NDEV * MICRO
    w1 = jax.random.normal(k1, (LAYERS, D, FF), jnp.float32) * (D ** -0.5)
    w2 = jax.random.normal(k2, (LAYERS, FF, D), jnp.float32) * ((FF * LAYERS) ** -0.5)
    x = jax.random.normal(k3, (rows, BATCH, SEQ, D), jnp.float32)
    dy = jax.random.normal(k4, (rows, BATCH, SEQ, D), jnp.float32) * ((rows * BATCH * SEQ) ** -0.25)
    return {"w1": w1.astype(jnp.bfloat16), "w2": w2.astype(jnp.bfloat16), "x": x.astype(jnp.bfloat16), "dy": dy.astype(jnp.bfloat16)}


def reference(w1, w2, x, dy):
    tok = BATCH * SEQ

    def step(acc, inp):
        acc1, acc2 = acc
        xm, gm = inp
        h = xm.reshape(tok, D)
        g = gm.reshape(tok, D)
        hs = []
        us = []
        acts = []
        for l in range(LAYERS):
            u = jnp.dot(h, w1[l], preferred_element_type=jnp.float32).astype(jnp.bfloat16)
            act = gelu_pair(u.astype(jnp.float32))[0].astype(jnp.bfloat16)
            hs.append(h)
            us.append(u)
            acts.append(act)
            if l + 1 < LAYERS:
                h = (h.astype(jnp.float32) + jnp.dot(act, w2[l], preferred_element_type=jnp.float32)).astype(jnp.bfloat16)
        d1 = [None] * LAYERS
        d2 = [None] * LAYERS
        for l in reversed(range(LAYERS)):
            da = jnp.dot(g, w2[l].T, preferred_element_type=jnp.float32)
            du = (da * gelu_pair(us[l].astype(jnp.float32))[1]).astype(jnp.bfloat16)
            d2[l] = jnp.dot(acts[l].T, g, preferred_element_type=jnp.float32)
            d1[l] = jnp.dot(hs[l].T, du, preferred_element_type=jnp.float32)
            g = (g.astype(jnp.float32) + jnp.dot(du, w1[l].T, preferred_element_type=jnp.float32)).astype(jnp.bfloat16)
        return (acc1 + jnp.stack(d1), acc2 + jnp.stack(d2)), g.reshape(BATCH, SEQ, D)

    init = (jnp.zeros((LAYERS, D, FF), jnp.float32), jnp.zeros((LAYERS, FF, D), jnp.float32))
    (acc1, acc2), dxs = lax.scan(step, init, (x, dy))
    return acc1.astype(jnp.bfloat16), acc2.astype(jnp.bfloat16), dxs
```

```python
import functools

import jax
import jax.numpy as jnp
from jax import lax
from jax.experimental import pallas as pl
from jax.experimental.pallas import tpu as pltpu
from jax.sharding import PartitionSpec as P

GC = 0.7978845608028654
GA = 0.044715
AXES = ("rep", "data")
MESH = pl.DeviceIdType.MESH
BF16 = jnp.bfloat16
F32 = jnp.float32

UR, UC = 48, 128
TR = 384
COLOURS = 3
ORDERS = (("x", "y", "z"), ("y", "x", "z"), ("z", "x", "y"))
SUB = 8
NSL = 4
OFF_RS = (1, 2, 3)
OFF_AG = (6, 5, 4)
TICKS = 11


def gelu_pair(u):
    t = jnp.tanh(GC * (u + GA * u * u * u))
    val = 0.5 * u * (1.0 + t)
    der = 0.5 * (1.0 + t) + 0.5 * u * (1.0 - t * t) * GC * (1.0 + 3.0 * GA * u * u)
    return val, der


def sub_of(n, i):
    if n == 8:
        return max(0, i - 1)
    return (0, 1, 3)[i] if n == 4 else 1


class Comm:
    def __init__(self, sizes, ff, d, tok):
        self.sizes, self.ff, self.d, self.tok = sizes, ff, d, tok
        self.units = ff // UR * 2
        self.tiles = ff // TR
        self.tu = TR // UR * 2
        self.cw = d // 2 // COLOURS
        self.n = [[sizes[a] for a in o] for o in ORDERS]
        self.stride, self.off, total = [], [], 0
        for c in range(COLOURS):
            s, st, of = self.units, [], []
            for f in range(3):
                s //= self.n[c][f]
                st.append(s)
                of.append(total)
                total += self.n[c][f] - 1
            self.stride.append(st)
            self.off.append(of)
        self.total = total

    def slot_shapes(self):
        return [
            pltpu.VMEM((2, self.n[c][f] - 1, self.stride[c][f] // 2, UR, UC), BF16)
            for c in range(COLOURS)
            for f in range(3)
        ]


def half_of(direction, i):
    return i % 2 if direction == 0 else 1 - i % 2


def comm_kernel(cm, *refs):
    srcs = refs[: 2 * NSL]
    out = refs[2 * NSL]
    g, lr, lt, stage = refs[2 * NSL + 1 : 2 * NSL + 5]
    slots = refs[2 * NSL + 5 : 2 * NSL + 14]
    (rs_ss, rs_rs, ag_ss, ag_rs, rs_c1, rs_c2, ag_c1, ag_c2, x_ss, x_rs, ld, p_ss, p_rs, o_s) = refs[2 * NSL + 14 :]
    nx, ny, nz = cm.sizes["x"], cm.sizes["y"], cm.sizes["z"]
    rep = lax.axis_index("rep")
    dat = lax.axis_index("data")
    pos = {"z": rep // ny, "y": rep % ny, "x": dat // 2}
    core = dat % 2

    def device(dim, step):
        p = dict(pos)
        n = cm.sizes[dim]
        p[dim] = (pos[dim] + step + n) % n
        return {"rep": p["z"] * ny + p["y"], "data": p["x"] * 2 + core}

    nbr = {(a, s): device(a, s) for a in ("x", "y", "z") for s in (1, -1)}
    partner = {"rep": rep, "data": pos["x"] * 2 + (1 - core)}

    def neighbour(c, f, direction):
        return nbr[(ORDERS[c][f], 1 if direction == 0 else -1)]

    def sender(c, f, direction):
        return nbr[(ORDERS[c][f], -1 if direction == 0 else 1)]

    bases = []
    for c in range(COLOURS):
        b, bs = 0, []
        for f in range(3):
            bs.append(b)
            b = b + pos[ORDERS[c][f]] * cm.stride[c][f]
        bases.append(bs)

    def region(c, f, step, half):
        n, s = cm.n[c][f], cm.stride[c][f]
        owner = (pos[ORDERS[c][f]] + step + n) % n
        return bases[c][f] + owner * s + half * (s // 2)

    def rs_region(c, f, direction, i):
        k = cm.n[c][f] // 2 - (i + 1) // 2
        return region(c, f, k if direction == 0 else -k, half_of(direction, i))

    def ag_region(c, f, direction, i):
        k = i // 2
        return region(c, f, -k if direction == 0 else k, half_of(direction, i))

    def rs_copy(c, f, direction, i, q):
        h = cm.stride[c][f] // 2
        j = cm.off[c][f] + i
        return pltpu.make_async_remote_copy(
            src_ref=g.at[q, c, pl.ds(rs_region(c, f, direction, i), h)],
            dst_ref=slots[3 * c + f].at[direction, i],
            send_sem=rs_ss.at[direction, j],
            recv_sem=rs_rs.at[direction, j],
            device_id=neighbour(c, f, direction),
            device_id_type=MESH,
        )

    def ag_copy(c, f, direction, i, q):
        h = cm.stride[c][f] // 2
        j = cm.off[c][f] + i
        ref = g.at[q, c, pl.ds(ag_region(c, f, direction, i), h)]
        return pltpu.make_async_remote_copy(
            src_ref=ref,
            dst_ref=ref,
            send_sem=ag_ss.at[direction, j],
            recv_sem=ag_rs.at[direction, j],
            device_id=neighbour(c, f, direction),
            device_id_type=MESH,
        )

    def push(c, start, count, q):
        ref = g.at[q, c, pl.ds(start, count)]
        there = out.at[q, core, c, pl.ds(start, count)]
        pltpu.make_async_remote_copy(
            src_ref=ref, dst_ref=there, send_sem=p_ss.at[q, c], recv_sem=p_rs.at[q, c], device_id=partner, device_id_type=MESH
        ).start()
        pltpu.make_async_copy(ref, there, o_s.at[q, c]).start()

    def signal(sem, dev):
        pl.semaphore_signal(sem, inc=1, device_id=dev, device_id_type=MESH)

    def sem3(ref, c, f, direction):
        return ref.at[3 * c + f, direction]

    def add_units(c, start, h, parts, q):
        b = min(8, h)

        def one(j, carry):
            at = start + j * b
            v = g[q, c, pl.ds(at, b)].astype(F32)
            for slot, direction, m in parts:
                v = v + slot[direction, m, pl.ds(j * b, b)].astype(F32)
            g[q, c, pl.ds(at, b)] = v.astype(BF16)
            return carry

        if h == b:
            one(0, 0)
        else:
            lax.fori_loop(0, h // b, one, 0)

    def rs_step(c, f, i, q):
        n, h = cm.n[c][f], cm.stride[c][f] // 2
        for direction in (0, 1):
            if i >= 2:
                rs_copy(c, f, direction, i - 2, q).wait_recv()
                add_units(c, rs_region(c, f, direction, i), h, [(slots[3 * c + f], direction, i - 2)], q)

            @pl.when(q >= 1)
            def _():
                if i == 0 and n >= 4:
                    pl.semaphore_wait(sem3(rs_c1, c, f, direction), 1)
                if i == max(n - 3, 0):
                    pl.semaphore_wait(sem3(rs_c2, c, f, direction), 1)

            rs_copy(c, f, direction, i, q).start()

    def ag_step(c, f, i, q):
        n, h = cm.n[c][f], cm.stride[c][f] // 2
        if f == 0 and i == 0:
            push(c, region(c, f, 0, 0), 2 * h, q)
        for direction in (0, 1):
            if i >= 2:
                ag_copy(c, f, direction, i - 2, q).wait_recv()
            if i == 0:
                pl.semaphore_wait(sem3(ag_c1, c, f, direction), 1)
            if i == max(n - 3, 0):

                @pl.when(q >= 1)
                def _():
                    pl.semaphore_wait(sem3(ag_c2, c, f, direction), 1)

            ag_copy(c, f, direction, i, q).start()
            if f == 0 and i >= 2:
                push(c, ag_region(c, f, direction, i), h, q)

    def early_sends(c, f, q, copy):
        for i in range(min(2, cm.n[c][f] - 1)):
            for direction in (0, 1):
                copy(c, f, direction, i, q).wait_send()

    def late_sends(c, f, q, copy):
        for i in range(2, cm.n[c][f] - 1):
            for direction in (0, 1):
                copy(c, f, direction, i, q).wait_send()

    def rs_fin(c, f, q):
        n, h = cm.n[c][f], cm.stride[c][f] // 2
        parts = ([], [])
        for m in range(max(n - 3, 0), n - 1):
            for direction in (0, 1):
                rs_copy(c, f, direction, m, q).wait_recv()
                parts[half_of(direction, m)].append((slots[3 * c + f], direction, m))
        for half in (0, 1):
            add_units(c, region(c, f, 0, half), h, parts[half], q)
        late_sends(c, f, q, rs_copy)

        @pl.when(q < NSL - 1)
        def _():
            for direction in (0, 1):
                signal(sem3(rs_c2, c, f, direction), sender(c, f, direction))

    def ag_fin(c, f, q):
        n, h = cm.n[c][f], cm.stride[c][f] // 2
        for m in range(max(n - 3, 0), n - 1):
            for direction in (0, 1):
                ag_copy(c, f, direction, m, q).wait_recv()
                if f == 0:
                    k = m // 2 + 1
                    push(c, region(c, f, -k if direction == 0 else k, half_of(direction, m)), h, q)
        late_sends(c, f, q, ag_copy)

        @pl.when(q < NSL - 1)
        def _():
            for direction in (0, 1):
                signal(sem3(ag_c2, c, f, direction), sender(c, f, direction))

    def load(q, par):
        return (
            pltpu.make_async_copy(srcs[2 * q], lr.at[par, :, pl.ds(0, cm.ff)], ld.at[par, 0]),
            pltpu.make_async_copy(srcs[2 * q + 1], lr.at[par, :, pl.ds(cm.ff, cm.d)], ld.at[par, 1]),
        )

    jt = cm.d // TR

    def compute(q, s):
        par = q % 2
        odd = q % 2

        def rows(tau):
            return pl.multiple_of((1 - odd) * tau * TR + odd * (cm.ff + (tau % jt) * TR), UC)

        def cols(tau, k, c):
            return pl.multiple_of((1 - odd) * cm.ff + odd * (tau // jt) * cm.d + k * (cm.d // 2) + c * cm.cw, UC)

        def x_copy(tau):
            return pltpu.make_async_remote_copy(
                src_ref=stage.at[tau % 2],
                dst_ref=g.at[q, :, pl.ds(tau * cm.tu, cm.tu)],
                send_sem=x_ss.at[tau % 2],
                recv_sem=x_rs.at[tau],
                device_id=partner,
                device_id_type=MESH,
            )

        def product(tau, k, c):
            r = lr[par, :, pl.ds(cols(tau, k, c), cm.cw)]
            return jnp.dot(lt[tau % 2], r, preferred_element_type=F32)

        def tile(t, carry):
            @pl.when(t < cm.tiles)
            def _():
                lt[t % 2] = lr[par, :, pl.ds(rows(t), TR)].T

                @pl.when(t >= 2)
                def _():
                    x_copy(t - 2).wait_send()

                def colour(c, carry):
                    v = product(t, 1 - core, c).astype(BF16)
                    for u in range(cm.tu):
                        stage[t % 2, c, u] = v[u // 2 * UR : u // 2 * UR + UR, u % 2 * UC : u % 2 * UC + UC]
                    return carry

                lax.fori_loop(0, COLOURS, colour, 0)
                x_copy(t).start()

            @pl.when(t >= 1)
            def _():
                tau = t - 1
                x_copy(tau).wait_recv()

                def colour(c, carry):
                    v = product(tau, core, c)
                    for u in range(cm.tu):
                        w = v[u // 2 * UR : u // 2 * UR + UR, u % 2 * UC : u % 2 * UC + UC]
                        w = w + g[q, c, tau * cm.tu + u].astype(F32)
                        g[q, c, tau * cm.tu + u] = w.astype(BF16)
                    return carry

                lax.fori_loop(0, COLOURS, colour, 0)

            return carry

        total = cm.tiles + 1
        lax.fori_loop(s * total // SUB, (s + 1) * total // SUB, tile, 0)
        if s == SUB - 1:
            for t in (cm.tiles - 2, cm.tiles - 1):
                x_copy(t).wait_send()

    barrier = pltpu.get_barrier_semaphore()
    peers = list(nbr.values()) + [partner]
    for dev in peers:
        signal(barrier, dev)
    for cp in load(0, 0):
        cp.start()
    pl.semaphore_wait(barrier, len(peers))

    def active(t, off):
        return (t >= off) & (t < off + NSL)

    def each(fn, f, q, cond=None):
        for c in range(COLOURS):
            fn(c, f, q)

    def steps(fn, f, s, q, only=None):
        for c in range(COLOURS):
            n = cm.n[c][f]
            for i in range(n - 1):
                if sub_of(n, i) == s:
                    fn(c, f, i, q)

    def tick(t, carry):
        for s in range(SUB):
            if s == 0:
                for q in range(1, NSL):

                    @pl.when(t + 1 == q)
                    def _(q=q):
                        for cp in load(q, q % 2):
                            cp.start()

                @pl.when(active(t, 0))
                def _():
                    for cp in load(0, t % 2):
                        cp.wait()

            for fn, f, off in ((rs_step, 0, OFF_RS[0]), (ag_step, 0, OFF_AG[0])):

                @pl.when(active(t, off))
                def _(fn=fn, f=f, off=off):
                    steps(fn, f, s, t - off)

            for fn, f, off in ((rs_step, 2, OFF_RS[2]), (ag_step, 2, OFF_AG[2]), (ag_step, 1, OFF_AG[1])):

                @pl.when(active(t, off))
                def _(fn=fn, f=f, off=off):
                    steps(fn, f, s, t - off)

            if s == 0:

                @pl.when(active(t, OFF_AG[0] + 1))
                def _():
                    each(ag_fin, 0, t - OFF_AG[0] - 1)

                @pl.when(active(t, OFF_RS[0] + 1))
                def _():
                    each(rs_fin, 0, t - OFF_RS[0] - 1)

            @pl.when(active(t, OFF_RS[1]))
            def _():
                steps(rs_step, 1, s, t - OFF_RS[1])

            @pl.when(active(t, 0))
            def _():
                compute(t, s)

            if s == SUB - 2:
                for f in range(3):

                    @pl.when(active(t, OFF_RS[f]))
                    def _(f=f):
                        q = t - OFF_RS[f]
                        for c in range(COLOURS):
                            early_sends(c, f, q, rs_copy)
                            if cm.n[c][f] >= 4:

                                @pl.when(q < NSL - 1)
                                def _(c=c):
                                    for direction in (0, 1):
                                        signal(sem3(rs_c1, c, f, direction), sender(c, f, direction))

                    @pl.when(active(t, OFF_AG[f]))
                    def _(f=f):
                        for c in range(COLOURS):
                            early_sends(c, f, t - OFF_AG[f], ag_copy)

            if s == SUB - 1:
                for f in (1, 2):

                    @pl.when(active(t, OFF_RS[f]))
                    def _(f=f):
                        each(rs_fin, f, t - OFF_RS[f])

                    @pl.when(active(t, OFF_AG[f]))
                    def _(f=f):
                        each(ag_fin, f, t - OFF_AG[f])

                for f in range(3):

                    @pl.when(active(t + 1, OFF_AG[f]))
                    def _(f=f):
                        for c in range(COLOURS):
                            for direction in (0, 1):
                                signal(sem3(ag_c1, c, f, direction), sender(c, f, direction))

        return carry

    lax.fori_loop(0, TICKS, tick, 0)
    for q in range(NSL):
        for c in range(COLOURS):
            cp = pltpu.make_async_remote_copy(
                src_ref=g.at[q, c],
                dst_ref=out.at[q, 1 - core, c],
                send_sem=p_ss.at[q, c],
                recv_sem=p_rs.at[q, c],
                device_id=partner,
                device_id_type=MESH,
            )
            cp.wait_send()
            cp.wait_recv()
            pltpu.make_async_copy(g.at[q, c], out.at[q, core, c], o_s.at[q, c]).wait()


def reduce_all(sizes, ff, d, tok, pieces):
    cm = Comm(sizes, ff, d, tok)
    dma = pltpu.SemaphoreType.DMA
    reg = pltpu.SemaphoreType.REGULAR
    any_spec = pl.BlockSpec(memory_space=pl.ANY)
    return pl.pallas_call(
        functools.partial(comm_kernel, cm),
        name="grad_sum",
        out_shape=jax.ShapeDtypeStruct((NSL, 2, COLOURS, cm.units, UR, UC), BF16),
        in_specs=[any_spec] * (2 * NSL),
        out_specs=any_spec,
        scratch_shapes=[
            pltpu.VMEM((NSL, COLOURS, cm.units, UR, UC), BF16),
            pltpu.VMEM((2, tok, ff + d), BF16),
            pltpu.VMEM((2, TR, tok), BF16),
            pltpu.VMEM((2, COLOURS, cm.tu, UR, UC), BF16),
        ]
        + cm.slot_shapes()
        + [dma((2, cm.total))] * 4
        + [reg((9, 2))] * 4
        + [dma((2,)), dma((cm.tiles,)), dma((2, 2))]
        + [dma((NSL, COLOURS))] * 3,
        compiler_params=pltpu.CompilerParams(collective_id=0, has_side_effects=True, vmem_limit_bytes=66_000_000),
        cost_estimate=pl.CostEstimate(flops=16 * tok * ff * d // 2, bytes_accessed=8 * ff * d, transcendentals=0),
    )(*pieces)


def place_kernel(tu, cw, o_ref, g_ref):
    for k in range(2):
        for c in range(COLOURS):
            for u in range(tu):
                at = k * COLOURS * cw + c * cw + u % 2 * UC
                g_ref[0, u // 2 * UR : u // 2 * UR + UR, at : at + UC] = o_ref[0, k, c, u]


def place(o, shape, q0, where):
    ff, d = max(shape[1:]), min(shape[1:])
    tu, cw = TR // UR * 2, d // 2 // COLOURS
    return pl.pallas_call(
        functools.partial(place_kernel, tu, cw),
        name="place",
        out_shape=jax.ShapeDtypeStruct(shape, BF16),
        grid=(shape[0], ff // TR),
        in_specs=[pl.BlockSpec((1, 2, COLOURS, tu, UR, UC), lambda l, t: (q0 - 2 * l, 0, 0, t, 0, 0))],
        out_specs=pl.BlockSpec((1, TR, d), where),
        compiler_params=pltpu.CompilerParams(dimension_semantics=("arbitrary", "arbitrary")),
        cost_estimate=pl.CostEstimate(flops=0, bytes_accessed=8 * ff * d, transcendentals=0),
    )(o)


def solution(mesh, sizes=None):
    if sizes is None:
        rep, data = mesh.shape["rep"], mesh.shape["data"]
        sizes = {"x": data // 2, "y": 4, "z": rep // 4}

    def local(w1, w2, x, dy):
        nl, nd, ff = w1.shape
        tok = x.shape[0] * x.shape[1] * x.shape[2]

        def mm(a, b):
            return jnp.dot(a, b, preferred_element_type=F32)

        h = x.reshape(tok, nd)
        g = dy.reshape(tok, nd)
        hs, us, acts = [], [], []
        for l in range(nl):
            u = mm(h, w1[l]).astype(BF16)
            act = gelu_pair(u.astype(F32))[0].astype(BF16)
            hs.append(h)
            us.append(u)
            acts.append(act)
            if l + 1 < nl:
                h = (h.astype(F32) + mm(act, w2[l])).astype(BF16)
        pieces = []
        for l in reversed(range(nl)):
            da = mm(g, w2[l].T)
            du = (da * gelu_pair(us[l].astype(F32))[1]).astype(BF16)
            pieces += [acts[l], g, du, hs[l]]
            g = (g.astype(F32) + mm(du, w1[l].T)).astype(BF16)
        o = reduce_all(sizes, ff, nd, tok, pieces)
        jt = nd // TR
        g1 = place(o, w1.shape, 3, lambda l, t: (l, t % jt, t // jt))
        g2 = place(o, w2.shape, 2, lambda l, t: (l, t, 0))
        return g1, g2, g.reshape(x.shape)

    return jax.shard_map(local, mesh=mesh, in_specs=(P(), P(), P(AXES), P(AXES)), out_specs=(P(), P(), P(AXES)), check_vma=False)
```

```python
import functools

import jax
import jax.numpy as jnp
from jax import lax
from jax.experimental import pallas as pl
from jax.experimental.pallas import tpu as pltpu
from jax.sharding import PartitionSpec as P

GC = 0.7978845608028654
GA = 0.044715
AXES = ("rep", "data")
MESH = pl.DeviceIdType.MESH
BF16 = jnp.bfloat16
F32 = jnp.float32

UR, UC = 48, 128
TR = 384
COLOURS = 3
ORDERS = (("x", "y", "z"), ("y", "x", "z"), ("z", "x", "y"))
SUB = 8
NSL = 4
OFF_DW = 0
OFF = {("rs", 0): 1, ("rs", 1): 2, ("rs", 2): 3, ("ag", 2): 4, ("ag", 1): 5, ("ag", 0): 6}
SEND = {
    ("rs", 0): {8: (0, 1, 2, 2, 3, 6, 7), 4: (0, 2, 4), 2: (1,)},
    ("rs", 1): {8: (-1, 6, 11, 9, 8, 6, 10), 4: (0, 0, 2), 2: (1,)},
    ("rs", 2): {8: (-1, 0, 1, 1, 2, 2, 5), 4: (1, 3, 4), 2: (1,)},
    ("ag", 2): {8: (0, 1, 2, 2, 3, 4, 5), 4: (0, 0, 4), 2: (1,)},
    ("ag", 1): {8: (1, -1, -2, 8, 2, 5, 8), 4: (-1, 0, 1), 2: (1,)},
    ("ag", 0): {8: (0, 0, 1, 2, 3, 6, 6), 4: (-2, 2, 3), 2: (1,)},
}
FIN = {("rs", 0): 8, ("rs", 1): 7, ("rs", 2): 7, ("ag", 2): 7, ("ag", 1): 5, ("ag", 0): 8}
EARLY = {("rs", 0): 6, ("rs", 1): 7, ("rs", 2): 7, ("ag", 2): 7, ("ag", 1): 3, ("ag", 0): 4}
CREDIT = {("rs", 0): 7, ("rs", 1): 5, ("rs", 2): 6, ("ag", 2): -1, ("ag", 1): -4, ("ag", 0): -2}
RANK = {
    "load": 0,
    ("send", "ag", 1): 1,
    ("early", "ag", 2): 2,
    ("send", "ag", 2): 3,
    ("send", "rs", 2): 4,
    ("send", "rs", 0): 5,
    ("send", "ag", 0): 6,
    ("fin", "ag", 2): 7,
    ("early", "rs", 1): 8,
    "chain": 9,
    ("fin", "rs", 1): 10,
    ("fin", "ag", 1): 11,
    ("credit", "ag", 1): 12,
    ("early", "ag", 1): 13,
    ("early", "ag", 0): 14,
    ("credit", "ag", 0): 15,
    ("fin", "rs", 0): 16,
    ("fin", "ag", 0): 17,
    ("early", "rs", 2): 18,
    ("credit", "rs", 1): 19,
    ("credit", "rs", 0): 20,
    ("fin", "rs", 2): 21,
    "dw": 22,
    ("send", "rs", 1): 24,
    ("credit", "rs", 2): 25,
    ("early", "rs", 0): 26,
    ("credit", "ag", 2): 27,
}
LATE = 23
CHAIN = {0: (0, 5), 1: (5, 12)}
DW = {1: (0, 1), 2: (1, 7), 3: (7, 9), 5: (9, 11), 6: (11, 16), 7: (16, 18)}
KT = 512
WB = 3
XB = 3
LAG = 2


def gelu_pair(u):
    t = jnp.tanh(GC * (u + GA * u * u * u))
    val = 0.5 * u * (1.0 + t)
    der = 0.5 * (1.0 + t) + 0.5 * u * (1.0 - t * t) * GC * (1.0 + 3.0 * GA * u * u)
    return val, der


class Comm:
    def __init__(self, sizes, ff, d, tok):
        self.sizes, self.ff, self.d, self.tok = sizes, ff, d, tok
        self.units = ff // UR * 2
        self.tiles = ff // TR
        self.tu = TR // UR * 2
        self.cw = d // 2 // COLOURS
        self.n = [[sizes[a] for a in o] for o in ORDERS]
        self.stride, self.off, total = [], [], 0
        for c in range(COLOURS):
            s, st, of = self.units, [], []
            for f in range(3):
                s //= self.n[c][f]
                st.append(s)
                of.append(total)
                total += self.n[c][f] - 1
            self.stride.append(st)
            self.off.append(of)
        self.total = total

    def slot_shapes(self):
        return [
            pltpu.VMEM((2, self.n[c][f] - 1, self.stride[c][f] // 2, UR, UC), BF16)
            for c in range(COLOURS)
            for f in range(3)
        ]


def half_of(direction, i):
    return i % 2 if direction == 0 else 1 - i % 2


def comm_kernel(cm, *refs):
    x_in, dy_in, h1_in, a1_in, a0_in, u1_in, u0_in, w1, w2, g, out, dx_out, lr, lt, stage, wb, ub, acc = refs[:18]
    slots = refs[18:27]
    (rs_ss, rs_rs, ag_ss, ag_rs, rs_c1, rs_c2, ag_c1, ag_c2, x_ss, x_rs, ld, p_ss, p_rs, w_s, u_s, d_s) = refs[27:]
    nx, ny, nz = cm.sizes["x"], cm.sizes["y"], cm.sizes["z"]
    rep = lax.axis_index("rep")
    dat = lax.axis_index("data")
    pos = {"z": rep // ny, "y": rep % ny, "x": dat // 2}
    core = dat % 2

    def device(dim, step):
        p = dict(pos)
        n = cm.sizes[dim]
        p[dim] = (pos[dim] + step + n) % n
        return {"rep": p["z"] * ny + p["y"], "data": p["x"] * 2 + core}

    nbr = {(a, s): device(a, s) for a in ("x", "y", "z") for s in (1, -1)}
    partner = {"rep": rep, "data": pos["x"] * 2 + (1 - core)}

    def neighbour(c, f, direction):
        return nbr[(ORDERS[c][f], 1 if direction == 0 else -1)]

    def sender(c, f, direction):
        return nbr[(ORDERS[c][f], -1 if direction == 0 else 1)]

    bases = []
    for c in range(COLOURS):
        b, bs = 0, []
        for f in range(3):
            bs.append(b)
            b = b + pos[ORDERS[c][f]] * cm.stride[c][f]
        bases.append(bs)

    def region(c, f, step, half):
        n, s = cm.n[c][f], cm.stride[c][f]
        owner = (pos[ORDERS[c][f]] + step + n) % n
        return bases[c][f] + owner * s + half * (s // 2)

    def rs_region(c, f, direction, i):
        k = cm.n[c][f] // 2 - (i + 1) // 2
        return region(c, f, k if direction == 0 else -k, half_of(direction, i))

    def ag_region(c, f, direction, i):
        k = i // 2
        return region(c, f, -k if direction == 0 else k, half_of(direction, i))

    def rs_copy(c, f, direction, i, q):
        h = cm.stride[c][f] // 2
        j = cm.off[c][f] + i
        return pltpu.make_async_remote_copy(
            src_ref=g.at[q, c, pl.ds(rs_region(c, f, direction, i), h)],
            dst_ref=slots[3 * c + f].at[direction, i],
            send_sem=rs_ss.at[direction, j],
            recv_sem=rs_rs.at[direction, j],
            device_id=neighbour(c, f, direction),
            device_id_type=MESH,
        )

    def ag_copy(c, f, direction, i, q):
        h = cm.stride[c][f] // 2
        j = cm.off[c][f] + i
        ref = g.at[q, c, pl.ds(ag_region(c, f, direction, i), h)]
        return pltpu.make_async_remote_copy(
            src_ref=ref,
            dst_ref=ref,
            send_sem=ag_ss.at[direction, j],
            recv_sem=ag_rs.at[direction, j],
            device_id=neighbour(c, f, direction),
            device_id_type=MESH,
        )

    def push(c, start, count, q):
        pltpu.make_async_remote_copy(
            src_ref=g.at[q, c, pl.ds(start, count)],
            dst_ref=out.at[q, c, pl.ds(start, count)],
            send_sem=p_ss.at[q, c],
            recv_sem=p_rs.at[q, c],
            device_id=partner,
            device_id_type=MESH,
        ).start()

    def signal(sem, dev):
        pl.semaphore_signal(sem, inc=1, device_id=dev, device_id_type=MESH)

    def sem3(ref, c, f, direction):
        return ref.at[3 * c + f, direction]

    def add_units(c, start, h, parts, q):
        b = min(8, h)

        def one(j, carry):
            at = start + j * b
            v = g[q, c, pl.ds(at, b)].astype(F32)
            for slot, direction, m in parts:
                v = v + slot[direction, m, pl.ds(j * b, b)].astype(F32)
            g[q, c, pl.ds(at, b)] = v.astype(BF16)
            return carry

        if h == b:
            one(0, 0)
        else:
            lax.fori_loop(0, h // b, one, 0)

    def rs_step(c, f, i, q):
        n, h = cm.n[c][f], cm.stride[c][f] // 2
        for direction in (0, 1):
            if i >= 2:
                rs_copy(c, f, direction, i - 2, q).wait_recv()
                add_units(c, rs_region(c, f, direction, i), h, [(slots[3 * c + f], direction, i - 2)], q)

            @pl.when(q >= 1)
            def _():
                if i == 0 and n >= 4:
                    pl.semaphore_wait(sem3(rs_c1, c, f, direction), 1)
                if i == max(n - 3, 0):
                    pl.semaphore_wait(sem3(rs_c2, c, f, direction), 1)

            rs_copy(c, f, direction, i, q).start()

    def ag_step(c, f, i, q):
        n, h = cm.n[c][f], cm.stride[c][f] // 2
        if f == 0 and i == 0:
            push(c, region(c, f, 0, 0), 2 * h, q)
        for direction in (0, 1):
            if i >= 2:
                ag_copy(c, f, direction, i - 2, q).wait_recv()
            if i == 0:
                pl.semaphore_wait(sem3(ag_c1, c, f, direction), 1)
            if i == max(n - 3, 0):

                @pl.when(q >= 1)
                def _():
                    pl.semaphore_wait(sem3(ag_c2, c, f, direction), 1)

            ag_copy(c, f, direction, i, q).start()
            if f == 0 and i >= 2:
                push(c, ag_region(c, f, direction, i), h, q)

    def early_sends(c, f, q, copy):
        for i in range(min(2, cm.n[c][f] - 1)):
            for direction in (0, 1):
                copy(c, f, direction, i, q).wait_send()

    def late_sends(c, f, q, copy):
        for i in range(2, cm.n[c][f] - 1):
            for direction in (0, 1):
                copy(c, f, direction, i, q).wait_send()

    def rs_fin(c, f, q):
        n, h = cm.n[c][f], cm.stride[c][f] // 2
        parts = ([], [])
        for m in range(max(n - 3, 0), n - 1):
            for direction in (0, 1):
                rs_copy(c, f, direction, m, q).wait_recv()
                parts[half_of(direction, m)].append((slots[3 * c + f], direction, m))
        for half in (0, 1):
            add_units(c, region(c, f, 0, half), h, parts[half], q)
        late_sends(c, f, q, rs_copy)

        @pl.when(q < NSL - 1)
        def _():
            for direction in (0, 1):
                signal(sem3(rs_c2, c, f, direction), sender(c, f, direction))

    def ag_fin(c, f, q):
        n, h = cm.n[c][f], cm.stride[c][f] // 2
        for m in range(max(n - 3, 0), n - 1):
            for direction in (0, 1):
                ag_copy(c, f, direction, m, q).wait_recv()
                if f == 0:
                    k = m // 2 + 1
                    push(c, region(c, f, -k if direction == 0 else k, half_of(direction, m)), h, q)
        late_sends(c, f, q, ag_copy)

        @pl.when(q < NSL - 1)
        def _():
            for direction in (0, 1):
                signal(sem3(ag_c2, c, f, direction), sender(c, f, direction))

    big, small = pl.ds(0, cm.ff), pl.ds(cm.ff, cm.d)
    loads = {
        "a1": (a1_in, 0, big),
        "dy": (dy_in, 0, small),
        "h1": (h1_in, 1, small),
        "a0": (a0_in, 0, big),
        "x": (x_in, 1, small),
    }

    def load(name):
        ref, par, where = loads[name]
        return pltpu.make_async_copy(ref, lr.at[par, :, where], ld.at[list(loads).index(name)])

    kt = cm.ff // KT
    kd = cm.d // KT

    def w_copy(job, k):
        l = 1 - job // 2
        if job % 2 == 0:
            rows = pl.ds(pl.multiple_of(k // kd * cm.d, cm.d), cm.d)
            src = w2.at[l, rows, pl.ds(pl.multiple_of(k % kd * KT, KT), KT)]
        else:
            src = w1.at[l, :, pl.ds(pl.multiple_of(k * KT, KT), KT)]
        return pltpu.make_async_copy(src, wb.at[k % WB], w_s.at[k % WB])

    def u_copy(job, n):
        at = pl.multiple_of(n * cm.d, cm.d)
        return pltpu.make_async_copy((u1_in if job < 2 else u0_in).at[:, pl.ds(at, cm.d)], ub, u_s)

    def dot_t(a, b):
        return lax.dot_general(a, b, (((1,), (1,)), ((), ())), preferred_element_type=F32)

    rb = 16

    def by_rows(fn):
        def rows16(r, carry):
            fn(pl.ds(pl.multiple_of(r * rb, rb), rb))
            return carry

        lax.fori_loop(0, cm.tok // rb, rows16, 0)

    def clear(at):
        acc[at, :] = jnp.zeros((rb, cm.d), F32)

    def g_end(at):
        lr[0, at, small] = (lr[0, at, small].astype(F32) + acc[at, :]).astype(BF16)

    def dx_copy():
        return pltpu.make_async_copy(lr.at[0, :, small], dx_out, d_s)

    def chain(job, lo, hi):
        odd = job % 2

        def one(k, carry):
            w_copy(0, k).wait()

            @pl.when(k + WB - 1 < kt)
            def _():
                for j in range(NSL):

                    @pl.when(job == j)
                    def _(j=j):
                        w_copy(j, k + WB - 1).start()

            for j in (0, 2):

                @pl.when((job == j) & (k % kd == 0))
                def _(j=j):
                    u_copy(j, k // kd).start()

            @pl.when((k == 0) | ((odd == 0) & (k % kd == 0)))
            def _():
                by_rows(clear)

            a = lr[odd, :, pl.ds(pl.multiple_of((1 - odd) * (cm.ff + k % kd * KT) + odd * k * KT, KT), KT)]
            for n in range(kd):
                at = pl.ds(n * KT, KT)
                acc[:, at] = acc[:, at] + dot_t(a, wb[k % WB, n * KT : n * KT + KT, :])

            @pl.when((odd == 0) & (k % kd == kd - 1))
            def _():
                u_copy(0, 0).wait()

                def du_rows(at):
                    v = acc[at, :] * gelu_pair(ub[at, :].astype(F32))[1]
                    lr[1, at, pl.ds(pl.multiple_of(k // kd * cm.d, cm.d), cm.d)] = v.astype(BF16)

                by_rows(du_rows)

            return carry

        lax.fori_loop(lo, hi, one, 0)
        if hi == kt:

            @pl.when(odd == 1)
            def _():
                by_rows(g_end)

            for j in range(1, NSL):

                @pl.when(job == j - 1)
                def _(j=j):
                    for k in range(WB - 1):
                        w_copy(j, k).start()

            @pl.when(job == NSL - 1)
            def _():
                dx_copy().start()

    def chain_loads(t):
        @pl.when(t == 1)
        def _():
            load("a0").start()

        @pl.when(t == 2)
        def _():
            load("a0").wait()
            load("x").start()

        @pl.when(t == 3)
        def _():
            load("x").wait()

    jt = cm.d // TR

    def compute(q, lo, hi):
        par = q % 2
        odd = q % 2

        def rows(tau):
            return pl.multiple_of((1 - odd) * tau * TR + odd * (cm.ff + (tau % jt) * TR), UC)

        def cols(tau, k, c):
            return pl.multiple_of((1 - odd) * cm.ff + odd * (tau // jt) * cm.d + k * (cm.d // 2) + c * cm.cw, UC)

        def x_copy(tau):
            return pltpu.make_async_remote_copy(
                src_ref=stage.at[tau % XB],
                dst_ref=g.at[q, :, pl.ds(tau * cm.tu, cm.tu)],
                send_sem=x_ss.at[tau % XB],
                recv_sem=x_rs.at[tau],
                device_id=partner,
                device_id_type=MESH,
            )

        def product(tau, k, c):
            r = lr[par, :, pl.ds(cols(tau, k, c), cm.cw)]
            return jnp.dot(lt[tau % XB], r, preferred_element_type=F32)

        def tile(t, carry):
            @pl.when(t < cm.tiles)
            def _():
                lt[t % XB] = lr[par, :, pl.ds(rows(t), TR)].T

                @pl.when(t >= XB)
                def _():
                    x_copy(t - XB).wait_send()

                def colour(c, carry):
                    v = product(t, 1 - core, c).astype(BF16)
                    for u in range(cm.tu):
                        stage[t % XB, c, u] = v[u // 2 * UR : u // 2 * UR + UR, u % 2 * UC : u % 2 * UC + UC]
                    return carry

                lax.fori_loop(0, COLOURS, colour, 0, unroll=True)
                x_copy(t).start()

            @pl.when(t >= LAG)
            def _():
                tau = t - LAG
                x_copy(tau).wait_recv()

                def colour(c, carry):
                    v = product(tau, core, c)
                    for u in range(cm.tu):
                        w = v[u // 2 * UR : u // 2 * UR + UR, u % 2 * UC : u % 2 * UC + UC]
                        w = w + g[q, c, tau * cm.tu + u].astype(F32)
                        g[q, c, tau * cm.tu + u] = w.astype(BF16)
                    return carry

                lax.fori_loop(0, COLOURS, colour, 0, unroll=True)

            return carry

        lax.fori_loop(lo, hi, tile, 0)
        if hi == cm.tiles + LAG:
            for t in range(max(cm.tiles - XB, 0), cm.tiles):
                x_copy(t).wait_send()

    barrier = pltpu.get_barrier_semaphore()
    peers = list(nbr.values()) + [partner]
    for dev in peers:
        signal(barrier, dev)
    for name in ("a1", "dy", "h1"):
        load(name).start()
    for k in range(WB - 1):
        w_copy(0, k).start()
    for name in ("a1", "dy", "h1"):
        load(name).wait()
    pl.semaphore_wait(barrier, len(peers))

    acts = []

    def act(at, rank, off, fn):
        acts.append((at % SUB, rank, off + at // SUB, fn))

    for key, off in OFF.items():
        kind, f = key
        step, fin, copy = (rs_step, rs_fin, rs_copy) if kind == "rs" else (ag_step, ag_fin, ag_copy)
        c1 = rs_c1 if kind == "rs" else ag_c1
        for c in range(COLOURS):
            n = cm.n[c][f]
            for i in range(n - 1):
                at = SEND[key][n][i]
                act(at, LATE if at < 0 else RANK[("send", *key)], off, functools.partial(step, c, f, i))
            act(FIN[key], RANK[("fin", *key)], off, functools.partial(fin, c, f))
            act(EARLY[key], RANK[("early", *key)], off, functools.partial(lambda c, f, copy, q: early_sends(c, f, q, copy), c, f, copy))

            def credit(c, f, kind, c1, q):
                def give():
                    for direction in (0, 1):
                        signal(sem3(c1, c, f, direction), sender(c, f, direction))

                if kind == "ag":
                    give()
                elif cm.n[c][f] >= 4:
                    pl.when(q < NSL - 1)(give)

            act(CREDIT[key], RANK[("credit", *key)], off, functools.partial(credit, c, f, kind, c1))
    for s, (lo, hi) in DW.items():
        act(s, RANK["dw"], OFF_DW, functools.partial(lambda lo, hi, q: compute(q, lo, hi), lo, hi))
    for s, (lo, hi) in CHAIN.items():
        act(s, RANK["chain"], OFF_DW + 1, functools.partial(lambda lo, hi, q: chain(q, lo, hi), lo, hi))
    acts.sort(key=lambda a: a[:3])
    ticks = max(a[2] for a in acts) + NSL

    def tick(t, carry):
        for s in range(SUB):
            if s == 0:
                chain_loads(t)
            mine = [a for a in acts if a[0] == s]
            while mine:
                first = mine[0][2]
                n = 0
                while n < len(mine) and mine[n][2] == first:
                    n += 1
                group, mine = mine[:n], mine[n:]

                @pl.when((t >= first) & (t < first + NSL))
                def _(group=group, first=first):
                    for _, _, _, fn in group:
                        fn(t - first)

        return carry

    lax.fori_loop(0, ticks, tick, 0)
    dx_copy().wait()
    for q in range(NSL):
        for c in range(COLOURS):
            cp = pltpu.make_async_remote_copy(
                src_ref=g.at[q, c],
                dst_ref=out.at[q, c],
                send_sem=p_ss.at[q, c],
                recv_sem=p_rs.at[q, c],
                device_id=partner,
                device_id_type=MESH,
            )
            cp.wait_send()
            cp.wait_recv()


def reduce_all(sizes, ff, d, tok, pieces):
    cm = Comm(sizes, ff, d, tok)
    dma = pltpu.SemaphoreType.DMA
    reg = pltpu.SemaphoreType.REGULAR
    any_spec = pl.BlockSpec(memory_space=pl.ANY)
    return pl.pallas_call(
        functools.partial(comm_kernel, cm),
        name="grad_sum",
        out_shape=(
            pltpu.VMEM((NSL, COLOURS, cm.units, UR, UC), BF16),
            jax.ShapeDtypeStruct((NSL, COLOURS, cm.units, UR, UC), BF16),
            jax.ShapeDtypeStruct((tok, d), BF16),
        ),
        in_specs=[any_spec] * 9,
        out_specs=(pl.BlockSpec(memory_space=pltpu.VMEM), any_spec, any_spec),
        scratch_shapes=[
            pltpu.VMEM((2, tok, ff + d), BF16),
            pltpu.VMEM((XB, TR, tok), BF16),
            pltpu.VMEM((XB, COLOURS, cm.tu, UR, UC), BF16),
            pltpu.VMEM((WB, d, KT), BF16),
            pltpu.VMEM((tok, d), BF16),
            pltpu.VMEM((tok, d), F32),
        ]
        + cm.slot_shapes()
        + [dma((2, cm.total))] * 4
        + [reg((9, 2))] * 4
        + [dma((XB,)), dma((cm.tiles,)), dma((5,))]
        + [dma((NSL, COLOURS))] * 2
        + [dma((WB,)), dma, dma],
        compiler_params=pltpu.CompilerParams(collective_id=0, has_side_effects=True, vmem_limit_bytes=26_500_000),
        cost_estimate=pl.CostEstimate(flops=16 * tok * ff * d // 2, bytes_accessed=8 * ff * d, transcendentals=0),
    )(*pieces)


BUFS = 8
AHEAD = 4


def place_kernel(tiles, ff, d, mine_ref, o_ref, g1_ref, g2_ref, buf, in_sem, out_sem, own_sem):
    cw = d // 2 // COLOURS
    tr = TR // UR
    jt = d // TR
    total = NSL * tiles
    core = lax.axis_index("data") % 2

    def fetch(j):
        q, tau = j // tiles, j % tiles
        return pltpu.make_async_copy(o_ref.at[q, :, pl.ds(tau * tr, tr)], buf.at[j % BUFS], in_sem.at[j % BUFS])

    def store(j, k, pieces, sem):
        q, tau = j // tiles, j % tiles
        l = 1 - q // 2
        for c in range(COLOURS):
            for h in range(2):
                col = k * (d // 2) + c * cw + h * UC

                @pl.when(q % 2 == 0)
                def _():
                    dst = g2_ref.at[l, pl.ds(tau * tr, tr), :, pl.ds(pl.multiple_of(col, UC), UC)]
                    pltpu.make_async_copy(pieces(c, h), dst, sem).start()

                @pl.when(q % 2 == 1)
                def _():
                    at = pl.multiple_of(tau // jt * d + col, UC)
                    dst = g1_ref.at[l, pl.ds(tau % jt * tr, tr), :, pl.ds(at, UC)]
                    pltpu.make_async_copy(pieces(c, h), dst, sem).start()

    def drain(j):
        b = j % BUFS
        pltpu.make_async_copy(buf.at[b], o_ref.at[0, :, pl.ds(0, tr)], out_sem.at[b]).wait()

    for j in range(AHEAD):
        fetch(j).start()

    def one(j, carry):
        q, tau = j // tiles, j % tiles
        store(j, core, lambda c, h: mine_ref.at[q, c, pl.ds(tau * tr, tr), h], own_sem)
        fetch(j).wait()
        store(j, 1 - core, lambda c, h: buf.at[j % BUFS, c, :, h], out_sem.at[j % BUFS])

        @pl.when(j + AHEAD < total)
        def _():
            @pl.when(j + AHEAD >= BUFS)
            def _():
                drain(j + AHEAD - BUFS)

            fetch(j + AHEAD).start()

        return carry

    lax.fori_loop(0, total, one, 0)
    for j in range(total - BUFS, total):
        drain(j)
    pltpu.make_async_copy(mine_ref, o_ref, own_sem).wait()


def place(mine, o, nl, ff, d):
    tiles = ff // TR
    any_spec = pl.BlockSpec(memory_space=pl.ANY)
    dma = pltpu.SemaphoreType.DMA
    shape = (NSL, COLOURS, ff // UR, 2, UR, UC)
    g1, g2 = pl.pallas_call(
        functools.partial(place_kernel, tiles, ff, d),
        name="place",
        out_shape=(
            jax.ShapeDtypeStruct((nl, d // UR, UR, ff), BF16),
            jax.ShapeDtypeStruct((nl, ff // UR, UR, d), BF16),
        ),
        in_specs=[any_spec, any_spec],
        out_specs=(any_spec, any_spec),
        scratch_shapes=[pltpu.VMEM((BUFS, COLOURS, TR // UR, 2, UR, UC), BF16), dma((BUFS,)), dma((BUFS,)), dma],
        compiler_params=pltpu.CompilerParams(vmem_limit_bytes=16_000_000),
        cost_estimate=pl.CostEstimate(flops=0, bytes_accessed=16 * ff * d, transcendentals=0),
    )(pltpu.with_memory_space_constraint(mine.reshape(shape), pltpu.VMEM), o.reshape(shape))
    return g1.reshape(nl, d, ff), g2.reshape(nl, ff, d)


def solution(mesh, sizes=None):
    if sizes is None:
        rep, data = mesh.shape["rep"], mesh.shape["data"]
        sizes = {"x": data // 2, "y": 4, "z": rep // 4}

    def local(w1, w2, x, dy):
        nl, nd, ff = w1.shape
        tok = x.shape[0] * x.shape[1] * x.shape[2]

        def mm(a, b):
            return jnp.dot(a, b, preferred_element_type=F32)

        h = x.reshape(tok, nd)
        g = dy.reshape(tok, nd)
        hs, us, acts = [], [], []
        for l in range(nl):
            u = mm(h, w1[l]).astype(BF16)
            act = gelu_pair(u.astype(F32))[0].astype(BF16)
            hs.append(h)
            us.append(u)
            acts.append(act)
            if l + 1 < nl:
                h = (h.astype(F32) + mm(act, w2[l])).astype(BF16)
        mine, o, dx = reduce_all(sizes, ff, nd, tok, [hs[0], g, hs[1], acts[1], acts[0], us[1], us[0], w1, w2])
        g1, g2 = place(mine, o, nl, ff, nd)
        return g1, g2, dx.reshape(x.shape)

    return jax.shard_map(local, mesh=mesh, in_specs=(P(), P(), P(AXES), P(AXES)), out_specs=(P(), P(), P(AXES)), check_vma=False)
```

```python
import functools

import jax
import jax.numpy as jnp
from jax import lax
from jax.experimental import pallas as pl
from jax.experimental.pallas import tpu as pltpu
from jax.sharding import PartitionSpec as P

GC = 0.7978845608028654
GA = 0.044715
AXES = ("rep", "data")
MESH = pl.DeviceIdType.MESH
BF16 = jnp.bfloat16
F32 = jnp.float32

UR, UC = 48, 128
TR = 384
COLOURS = 3
ORDERS = (("x", "y", "z"), ("y", "x", "z"), ("z", "x", "y"))
ODD_ORDERS = (("x", "y", "z"), ("y", "x", "z"), ("z", "y", "x"))
SUB = 8
NSL = 4
OFF_DW = 0
OFF = {("rs", 0): 1, ("rs", 1): 2, ("rs", 2): 3, ("ag", 2): 4, ("ag", 1): 5, ("ag", 0): 6}
SEND = {
    ("rs", 0): {8: (0, 1, 2, 2, 3, 6, 7), 4: (0, 2, 6), 2: (1,)},
    ("rs", 1): {8: (-4, 7, 14, 10, 10, 5, 9), 4: (0, 3, 3), 2: (1,)},
    ("rs", 2): {8: (-1, -1, 1, 1, 2, 2, 6), 4: (-1, 2, 2), 2: (1,)},
    ("ag", 2): {8: (-1, 1, 2, 2, 4, 5, 6), 4: (0, 0, 3), 2: (1,)},
    ("ag", 1): {8: (3, 0, -3, 7, 4, 9, 6), 4: (-1, -1, 3), 2: (1,)},
    ("ag", 0): {8: (-2, 0, 1, 1, 2, 4, 6), 4: (-2, 1, 3), 2: (1,)},
}
FIN = {("rs", 0): 8, ("rs", 1): 7, ("rs", 2): 6, ("ag", 2): 7, ("ag", 1): 6, ("ag", 0): 8}
EARLY = {("rs", 0): 7, ("rs", 1): 7, ("rs", 2): 6, ("ag", 2): 5, ("ag", 1): 4, ("ag", 0): 5}
CREDIT = {("rs", 0): 7, ("rs", 1): 7, ("rs", 2): 6, ("ag", 2): -2, ("ag", 1): -5, ("ag", 0): -2}
RANK = {
    "load": 0,
    ("fin", "rs", 1): 1,
    ("send", "rs", 2): 2,
    ("send", "rs", 0): 3,
    ("send", "ag", 1): 4,
    ("early", "ag", 2): 5,
    ("fin", "ag", 1): 6,
    ("send", "ag", 2): 7,
    ("fin", "ag", 2): 8,
    ("early", "ag", 1): 9,
    "chain": 10,
    ("send", "ag", 0): 11,
    ("credit", "rs", 1): 12,
    ("credit", "ag", 1): 13,
    ("credit", "ag", 0): 14,
    ("fin", "rs", 0): 15,
    ("credit", "rs", 0): 16,
    ("early", "rs", 1): 17,
    ("early", "rs", 2): 18,
    ("credit", "rs", 2): 19,
    ("early", "ag", 0): 20,
    ("early", "rs", 0): 21,
    ("fin", "ag", 0): 22,
    ("send", "rs", 1): 23,
    "dw": 24,
    ("fin", "rs", 2): 26,
    ("credit", "ag", 2): 27,
}
LATE = 25
CHAIN = {0: (0, 7), 1: (7, 12)}
DW = {1: (0, 2), 2: (2, 10), 4: (10, 12), 6: (12, 17), 7: (17, 18)}
KT = 512
WB = 3
XB = 3
LAG = 2


def gelu_pair(u):
    t = jnp.tanh(GC * (u + GA * u * u * u))
    val = 0.5 * u * (1.0 + t)
    der = 0.5 * (1.0 + t) + 0.5 * u * (1.0 - t * t) * GC * (1.0 + 3.0 * GA * u * u)
    return val, der


class Comm:
    def __init__(self, sizes, ff, d, tok):
        self.sizes, self.ff, self.d, self.tok = sizes, ff, d, tok
        self.units = ff // UR * 2
        self.tiles = ff // TR
        self.tu = TR // UR * 2
        self.cw = d // 2 // COLOURS
        self.n = [[sizes[a] for a in o] for o in ORDERS]
        self.stride, self.off, total = [], [], 0
        for c in range(COLOURS):
            s, st, of = self.units, [], []
            for f in range(3):
                s //= self.n[c][f]
                st.append(s)
                of.append(total)
                total += self.n[c][f] - 1
            self.stride.append(st)
            self.off.append(of)
        self.total = total

    def slot_shapes(self):
        return [
            pltpu.VMEM((2, self.n[c][f] - 1, self.stride[c][f] // 2, UR, UC), BF16)
            for c in range(COLOURS)
            for f in range(3)
        ]


def half_of(direction, i):
    return i % 2 if direction == 0 else 1 - i % 2


def comm_kernel(cm, *refs):
    x_in, dy_in, h1_in, a1_in, a0_in, u1_in, u0_in, w1, w2, g, out, dx_out, lr, lt, stage, wb, ub, acc = refs[:18]
    slots = refs[18:27]
    (rs_ss, rs_rs, ag_ss, ag_rs, rs_c1, rs_c2, ag_c1, ag_c2, x_ss, x_rs, ld, p_ss, p_rs, w_s, u_s, d_s) = refs[27:]
    nx, ny, nz = cm.sizes["x"], cm.sizes["y"], cm.sizes["z"]
    rep = lax.axis_index("rep")
    dat = lax.axis_index("data")
    pos = {"z": rep // ny, "y": rep % ny, "x": dat // 2}
    core = dat % 2

    def device(dim, step):
        p = dict(pos)
        n = cm.sizes[dim]
        p[dim] = (pos[dim] + step + n) % n
        return {"rep": p["z"] * ny + p["y"], "data": p["x"] * 2 + core}

    nbr = {(a, s): device(a, s) for a in ("x", "y", "z") for s in (1, -1)}
    partner = {"rep": rep, "data": pos["x"] * 2 + (1 - core)}

    def either(q, even, odd):
        return even * (1 - q % 2) + odd * (q % 2)

    def beside(c, f, step, q):
        a, b = nbr[(ORDERS[c][f], step)], nbr[(ODD_ORDERS[c][f], step)]
        return a if a is b else {k: either(q, a[k], b[k]) for k in a}

    def neighbour(c, f, direction, q):
        return beside(c, f, 1 if direction == 0 else -1, q)

    def sender(c, f, direction, q):
        return beside(c, f, -1 if direction == 0 else 1, q)

    def place_on(c, f, q):
        a, b = ORDERS[c][f], ODD_ORDERS[c][f]
        return pos[a] if a == b else either(q, pos[a], pos[b])

    def region(c, f, step, half, q):
        n, s = cm.n[c][f], cm.stride[c][f]
        owner = (place_on(c, f, q) + step + n) % n
        at = owner * s + half * (s // 2)
        for e in range(f):
            at = at + place_on(c, e, q) * cm.stride[c][e]
        return at

    def rs_region(c, f, direction, i, q):
        k = cm.n[c][f] // 2 - (i + 1) // 2
        return region(c, f, k if direction == 0 else -k, half_of(direction, i), q)

    def ag_region(c, f, direction, i, q):
        k = i // 2
        return region(c, f, -k if direction == 0 else k, half_of(direction, i), q)

    def rs_copy(c, f, direction, i, q):
        h = cm.stride[c][f] // 2
        j = cm.off[c][f] + i
        return pltpu.make_async_remote_copy(
            src_ref=g.at[q, c, pl.ds(rs_region(c, f, direction, i, q), h)],
            dst_ref=slots[3 * c + f].at[direction, i],
            send_sem=rs_ss.at[direction, j],
            recv_sem=rs_rs.at[direction, j],
            device_id=neighbour(c, f, direction, q),
            device_id_type=MESH,
        )

    def ag_copy(c, f, direction, i, q):
        h = cm.stride[c][f] // 2
        j = cm.off[c][f] + i
        ref = g.at[q, c, pl.ds(ag_region(c, f, direction, i, q), h)]
        return pltpu.make_async_remote_copy(
            src_ref=ref,
            dst_ref=ref,
            send_sem=ag_ss.at[direction, j],
            recv_sem=ag_rs.at[direction, j],
            device_id=neighbour(c, f, direction, q),
            device_id_type=MESH,
        )

    def push(c, start, count, q):
        pltpu.make_async_remote_copy(
            src_ref=g.at[q, c, pl.ds(start, count)],
            dst_ref=out.at[q, c, pl.ds(start, count)],
            send_sem=p_ss.at[q, c],
            recv_sem=p_rs.at[q, c],
            device_id=partner,
            device_id_type=MESH,
        ).start()

    def signal(sem, dev):
        pl.semaphore_signal(sem, inc=1, device_id=dev, device_id_type=MESH)

    def sem3(ref, c, f, direction, q):
        return ref.at[3 * c + f, direction, q % 2]

    def add_units(c, start, h, parts, q):
        b = min(8, h)

        def one(j, carry):
            at = start + j * b
            v = g[q, c, pl.ds(at, b)].astype(F32)
            for slot, direction, m in parts:
                v = v + slot[direction, m, pl.ds(j * b, b)].astype(F32)
            g[q, c, pl.ds(at, b)] = v.astype(BF16)
            return carry

        if h == b:
            one(0, 0)
        else:
            lax.fori_loop(0, h // b, one, 0)

    def rs_step(c, f, i, q):
        n, h = cm.n[c][f], cm.stride[c][f] // 2
        for direction in (0, 1):
            if i >= 2:
                rs_copy(c, f, direction, i - 2, q).wait_recv()
                add_units(c, rs_region(c, f, direction, i, q), h, [(slots[3 * c + f], direction, i - 2)], q)

            @pl.when(q >= 1)
            def _():
                if i == 0 and n >= 4:
                    pl.semaphore_wait(sem3(rs_c1, c, f, direction, q), 1)
                if i == max(n - 3, 0):
                    pl.semaphore_wait(sem3(rs_c2, c, f, direction, q), 1)

            rs_copy(c, f, direction, i, q).start()

    def ag_step(c, f, i, q):
        n, h = cm.n[c][f], cm.stride[c][f] // 2
        if f == 0 and i == 0:
            push(c, region(c, f, 0, 0, q), 2 * h, q)
        for direction in (0, 1):
            if i >= 2:
                ag_copy(c, f, direction, i - 2, q).wait_recv()
            if i == 0:
                pl.semaphore_wait(sem3(ag_c1, c, f, direction, q), 1)
            if i == max(n - 3, 0):

                @pl.when(q >= 1)
                def _():
                    pl.semaphore_wait(sem3(ag_c2, c, f, direction, q), 1)

            ag_copy(c, f, direction, i, q).start()
            if f == 0 and i >= 2:
                push(c, ag_region(c, f, direction, i, q), h, q)

    def early_sends(c, f, q, copy):
        for i in range(min(2, cm.n[c][f] - 1)):
            for direction in (0, 1):
                copy(c, f, direction, i, q).wait_send()

    def late_sends(c, f, q, copy):
        for i in range(2, cm.n[c][f] - 1):
            for direction in (0, 1):
                copy(c, f, direction, i, q).wait_send()

    def rs_fin(c, f, q):
        n, h = cm.n[c][f], cm.stride[c][f] // 2
        parts = ([], [])
        for m in range(max(n - 3, 0), n - 1):
            for direction in (0, 1):
                rs_copy(c, f, direction, m, q).wait_recv()
                parts[half_of(direction, m)].append((slots[3 * c + f], direction, m))
        for half in (0, 1):
            add_units(c, region(c, f, 0, half, q), h, parts[half], q)
        late_sends(c, f, q, rs_copy)

        @pl.when(q < NSL - 1)
        def _():
            for direction in (0, 1):
                signal(sem3(rs_c2, c, f, direction, q + 1), sender(c, f, direction, q + 1))

    def ag_fin(c, f, q):
        n, h = cm.n[c][f], cm.stride[c][f] // 2
        for m in range(max(n - 3, 0), n - 1):
            for direction in (0, 1):
                ag_copy(c, f, direction, m, q).wait_recv()
                if f == 0:
                    k = m // 2 + 1
                    push(c, region(c, f, -k if direction == 0 else k, half_of(direction, m), q), h, q)
        late_sends(c, f, q, ag_copy)

        @pl.when(q < NSL - 1)
        def _():
            for direction in (0, 1):
                signal(sem3(ag_c2, c, f, direction, q + 1), sender(c, f, direction, q + 1))

    big, small = pl.ds(0, cm.ff), pl.ds(cm.ff, cm.d)
    loads = {
        "a1": (a1_in, 0, big),
        "dy": (dy_in, 0, small),
        "h1": (h1_in, 1, small),
        "a0": (a0_in, 0, big),
        "x": (x_in, 1, small),
    }

    def load(name):
        ref, par, where = loads[name]
        return pltpu.make_async_copy(ref, lr.at[par, :, where], ld.at[list(loads).index(name)])

    kt = cm.ff // KT
    kd = cm.d // KT

    def w_copy(job, k):
        l = 1 - job // 2
        if job % 2 == 0:
            rows = pl.ds(pl.multiple_of(k // kd * cm.d, cm.d), cm.d)
            src = w2.at[l, rows, pl.ds(pl.multiple_of(k % kd * KT, KT), KT)]
        else:
            src = w1.at[l, :, pl.ds(pl.multiple_of(k * KT, KT), KT)]
        return pltpu.make_async_copy(src, wb.at[k % WB], w_s.at[k % WB])

    def u_copy(job, n):
        at = pl.multiple_of(n * cm.d, cm.d)
        return pltpu.make_async_copy((u1_in if job < 2 else u0_in).at[:, pl.ds(at, cm.d)], ub, u_s)

    def dot_t(a, b):
        return lax.dot_general(a, b, (((1,), (1,)), ((), ())), preferred_element_type=F32)

    rb = 16

    def by_rows(fn):
        def rows16(r, carry):
            fn(pl.ds(pl.multiple_of(r * rb, rb), rb))
            return carry

        lax.fori_loop(0, cm.tok // rb, rows16, 0)

    def clear(at):
        acc[at, :] = jnp.zeros((rb, cm.d), F32)

    def g_end(at):
        lr[0, at, small] = (lr[0, at, small].astype(F32) + acc[at, :]).astype(BF16)

    def dx_copy():
        return pltpu.make_async_copy(lr.at[0, :, small], dx_out, d_s)

    def chain(job, lo, hi):
        odd = job % 2

        def one(k, carry):
            w_copy(0, k).wait()

            @pl.when(k + WB - 1 < kt)
            def _():
                for j in range(NSL):

                    @pl.when(job == j)
                    def _(j=j):
                        w_copy(j, k + WB - 1).start()

            for j in (0, 2):

                @pl.when((job == j) & (k % kd == 0))
                def _(j=j):
                    u_copy(j, k // kd).start()

            @pl.when((k == 0) | ((odd == 0) & (k % kd == 0)))
            def _():
                by_rows(clear)

            a = lr[odd, :, pl.ds(pl.multiple_of((1 - odd) * (cm.ff + k % kd * KT) + odd * k * KT, KT), KT)]
            for n in range(kd):
                at = pl.ds(n * KT, KT)
                acc[:, at] = acc[:, at] + dot_t(a, wb[k % WB, n * KT : n * KT + KT, :])

            @pl.when((odd == 0) & (k % kd == kd - 1))
            def _():
                u_copy(0, 0).wait()

                def du_rows(at):
                    v = acc[at, :] * gelu_pair(ub[at, :].astype(F32))[1]
                    lr[1, at, pl.ds(pl.multiple_of(k // kd * cm.d, cm.d), cm.d)] = v.astype(BF16)

                by_rows(du_rows)

            return carry

        lax.fori_loop(lo, hi, one, 0)
        if hi == kt:

            @pl.when(odd == 1)
            def _():
                by_rows(g_end)

            for j in range(1, NSL):

                @pl.when(job == j - 1)
                def _(j=j):
                    for k in range(WB - 1):
                        w_copy(j, k).start()

            @pl.when(job == NSL - 1)
            def _():
                dx_copy().start()

    def chain_loads(t):
        @pl.when(t == 1)
        def _():
            load("a0").start()

        @pl.when(t == 2)
        def _():
            load("a0").wait()
            load("x").start()

        @pl.when(t == 3)
        def _():
            load("x").wait()

    jt = cm.d // TR

    def compute(q, lo, hi):
        par = q % 2
        odd = q % 2

        def rows(tau):
            return pl.multiple_of((1 - odd) * tau * TR + odd * (cm.ff + (tau % jt) * TR), UC)

        def cols(tau, k, c):
            return pl.multiple_of((1 - odd) * cm.ff + odd * (tau // jt) * cm.d + k * (cm.d // 2) + c * cm.cw, UC)

        def x_copy(tau):
            return pltpu.make_async_remote_copy(
                src_ref=stage.at[tau % XB],
                dst_ref=g.at[q, :, pl.ds(tau * cm.tu, cm.tu)],
                send_sem=x_ss.at[tau % XB],
                recv_sem=x_rs.at[tau],
                device_id=partner,
                device_id_type=MESH,
            )

        def product(tau, k, c):
            r = lr[par, :, pl.ds(cols(tau, k, c), cm.cw)]
            return jnp.dot(lt[tau % XB], r, preferred_element_type=F32)

        def tile(t, carry):
            @pl.when(t < cm.tiles)
            def _():
                lt[t % XB] = lr[par, :, pl.ds(rows(t), TR)].T

                @pl.when(t >= XB)
                def _():
                    x_copy(t - XB).wait_send()

                def colour(c, carry):
                    v = product(t, 1 - core, c).astype(BF16)
                    for u in range(cm.tu):
                        stage[t % XB, c, u] = v[u // 2 * UR : u // 2 * UR + UR, u % 2 * UC : u % 2 * UC + UC]
                    return carry

                lax.fori_loop(0, COLOURS, colour, 0, unroll=True)
                x_copy(t).start()

            @pl.when(t >= LAG)
            def _():
                tau = t - LAG
                x_copy(tau).wait_recv()

                def colour(c, carry):
                    v = product(tau, core, c)
                    for u in range(cm.tu):
                        w = v[u // 2 * UR : u // 2 * UR + UR, u % 2 * UC : u % 2 * UC + UC]
                        w = w + g[q, c, tau * cm.tu + u].astype(F32)
                        g[q, c, tau * cm.tu + u] = w.astype(BF16)
                    return carry

                lax.fori_loop(0, COLOURS, colour, 0, unroll=True)

            return carry

        lax.fori_loop(lo, hi, tile, 0)
        if hi == cm.tiles + LAG:
            for t in range(max(cm.tiles - XB, 0), cm.tiles):
                x_copy(t).wait_send()

    barrier = pltpu.get_barrier_semaphore()
    peers = list(nbr.values()) + [partner]
    for dev in peers:
        signal(barrier, dev)
    for name in ("a1", "dy", "h1"):
        load(name).start()
    for k in range(WB - 1):
        w_copy(0, k).start()
    for name in ("a1", "dy", "h1"):
        load(name).wait()
    pl.semaphore_wait(barrier, len(peers))

    acts = []

    def act(at, rank, off, fn):
        acts.append((at % SUB, rank, off + at // SUB, fn))

    for key, off in OFF.items():
        kind, f = key
        step, fin, copy = (rs_step, rs_fin, rs_copy) if kind == "rs" else (ag_step, ag_fin, ag_copy)
        c1 = rs_c1 if kind == "rs" else ag_c1
        for c in range(COLOURS):
            n = cm.n[c][f]
            for i in range(n - 1):
                at = SEND[key][n][i]
                act(at, LATE if at < 0 else RANK[("send", *key)], off, functools.partial(step, c, f, i))
            act(FIN[key], RANK[("fin", *key)], off, functools.partial(fin, c, f))
            act(EARLY[key], RANK[("early", *key)], off, functools.partial(lambda c, f, copy, q: early_sends(c, f, q, copy), c, f, copy))

            def credit(c, f, kind, c1, q):
                def give():
                    for direction in (0, 1):
                        r = q if kind == "ag" else q + 1
                        signal(sem3(c1, c, f, direction, r), sender(c, f, direction, r))

                if kind == "ag":
                    give()
                elif cm.n[c][f] >= 4:
                    pl.when(q < NSL - 1)(give)

            act(CREDIT[key], RANK[("credit", *key)], off, functools.partial(credit, c, f, kind, c1))
    for s, (lo, hi) in DW.items():
        act(s, RANK["dw"], OFF_DW, functools.partial(lambda lo, hi, q: compute(q, lo, hi), lo, hi))
    for s, (lo, hi) in CHAIN.items():
        act(s, RANK["chain"], OFF_DW + 1, functools.partial(lambda lo, hi, q: chain(q, lo, hi), lo, hi))
    acts.sort(key=lambda a: a[:3])
    ticks = max(a[2] for a in acts) + NSL

    def tick(t, carry):
        for s in range(SUB):
            if s == 0:
                chain_loads(t)
            mine = [a for a in acts if a[0] == s]
            while mine:
                first = mine[0][2]
                n = 0
                while n < len(mine) and mine[n][2] == first:
                    n += 1
                group, mine = mine[:n], mine[n:]

                @pl.when((t >= first) & (t < first + NSL))
                def _(group=group, first=first):
                    for _, _, _, fn in group:
                        fn(t - first)

        return carry

    lax.fori_loop(0, ticks, tick, 0)
    dx_copy().wait()
    for q in range(NSL):
        for c in range(COLOURS):
            cp = pltpu.make_async_remote_copy(
                src_ref=g.at[q, c],
                dst_ref=out.at[q, c],
                send_sem=p_ss.at[q, c],
                recv_sem=p_rs.at[q, c],
                device_id=partner,
                device_id_type=MESH,
            )
            cp.wait_send()
            cp.wait_recv()


def reduce_all(sizes, ff, d, tok, pieces):
    cm = Comm(sizes, ff, d, tok)
    dma = pltpu.SemaphoreType.DMA
    reg = pltpu.SemaphoreType.REGULAR
    any_spec = pl.BlockSpec(memory_space=pl.ANY)
    return pl.pallas_call(
        functools.partial(comm_kernel, cm),
        name="grad_sum",
        out_shape=(
            pltpu.VMEM((NSL, COLOURS, cm.units, UR, UC), BF16),
            jax.ShapeDtypeStruct((NSL, COLOURS, cm.units, UR, UC), BF16),
            jax.ShapeDtypeStruct((tok, d), BF16),
        ),
        in_specs=[any_spec] * 9,
        out_specs=(pl.BlockSpec(memory_space=pltpu.VMEM), any_spec, any_spec),
        scratch_shapes=[
            pltpu.VMEM((2, tok, ff + d), BF16),
            pltpu.VMEM((XB, TR, tok), BF16),
            pltpu.VMEM((XB, COLOURS, cm.tu, UR, UC), BF16),
            pltpu.VMEM((WB, d, KT), BF16),
            pltpu.VMEM((tok, d), BF16),
            pltpu.VMEM((tok, d), F32),
        ]
        + cm.slot_shapes()
        + [dma((2, cm.total))] * 4
        + [reg((9, 2, 2))] * 4
        + [dma((XB,)), dma((cm.tiles,)), dma((5,))]
        + [dma((NSL, COLOURS))] * 2
        + [dma((WB,)), dma, dma],
        compiler_params=pltpu.CompilerParams(collective_id=0, has_side_effects=True, vmem_limit_bytes=26_500_000),
        cost_estimate=pl.CostEstimate(flops=16 * tok * ff * d // 2, bytes_accessed=8 * ff * d, transcendentals=0),
    )(*pieces)


BUFS = 16
AHEAD = 12


def place_kernel(tiles, ff, d, mine_ref, o_ref, g1_ref, g2_ref, buf, in_sem, out_sem, own_sem):
    cw = d // 2 // COLOURS
    tr = TR // UR
    jt = d // TR
    total = NSL * tiles
    core = lax.axis_index("data") % 2

    def fetch(j):
        q, tau = j // tiles, j % tiles
        return pltpu.make_async_copy(o_ref.at[q, :, pl.ds(tau * tr, tr)], buf.at[j % BUFS], in_sem.at[j % BUFS])

    def store(j, k, pieces, sem):
        q, tau = j // tiles, j % tiles
        l = 1 - q // 2
        for c in range(COLOURS):
            for h in range(2):
                col = k * (d // 2) + c * cw + h * UC

                @pl.when(q % 2 == 0)
                def _():
                    dst = g2_ref.at[l, pl.ds(tau * tr, tr), :, pl.ds(pl.multiple_of(col, UC), UC)]
                    pltpu.make_async_copy(pieces(c, h), dst, sem).start()

                @pl.when(q % 2 == 1)
                def _():
                    at = pl.multiple_of(tau // jt * d + col, UC)
                    dst = g1_ref.at[l, pl.ds(tau % jt * tr, tr), :, pl.ds(at, UC)]
                    pltpu.make_async_copy(pieces(c, h), dst, sem).start()

    def drain(j):
        b = j % BUFS
        pltpu.make_async_copy(buf.at[b], o_ref.at[0, :, pl.ds(0, tr)], out_sem.at[b]).wait()

    for j in range(AHEAD):
        fetch(j).start()

    def one(j, carry):
        q, tau = j // tiles, j % tiles
        store(j, core, lambda c, h: mine_ref.at[q, c, pl.ds(tau * tr, tr), h], own_sem)
        fetch(j).wait()
        store(j, 1 - core, lambda c, h: buf.at[j % BUFS, c, :, h], out_sem.at[j % BUFS])

        @pl.when(j + AHEAD < total)
        def _():
            @pl.when(j + AHEAD >= BUFS)
            def _():
                drain(j + AHEAD - BUFS)

            fetch(j + AHEAD).start()

        return carry

    lax.fori_loop(0, total, one, 0)
    for j in range(total - BUFS, total):
        drain(j)
    pltpu.make_async_copy(mine_ref, o_ref, own_sem).wait()


def place(mine, o, nl, ff, d):
    tiles = ff // TR
    any_spec = pl.BlockSpec(memory_space=pl.ANY)
    dma = pltpu.SemaphoreType.DMA
    shape = (NSL, COLOURS, ff // UR, 2, UR, UC)
    g1, g2 = pl.pallas_call(
        functools.partial(place_kernel, tiles, ff, d),
        name="place",
        out_shape=(
            jax.ShapeDtypeStruct((nl, d // UR, UR, ff), BF16),
            jax.ShapeDtypeStruct((nl, ff // UR, UR, d), BF16),
        ),
        in_specs=[any_spec, any_spec],
        out_specs=(any_spec, any_spec),
        scratch_shapes=[pltpu.VMEM((BUFS, COLOURS, TR // UR, 2, UR, UC), BF16), dma((BUFS,)), dma((BUFS,)), dma],
        compiler_params=pltpu.CompilerParams(vmem_limit_bytes=16_000_000),
        cost_estimate=pl.CostEstimate(flops=0, bytes_accessed=16 * ff * d, transcendentals=0),
    )(pltpu.with_memory_space_constraint(mine.reshape(shape), pltpu.VMEM), o.reshape(shape))
    return g1.reshape(nl, d, ff), g2.reshape(nl, ff, d)


def solution(mesh, sizes=None):
    if sizes is None:
        rep, data = mesh.shape["rep"], mesh.shape["data"]
        sizes = {"x": data // 2, "y": 4, "z": rep // 4}

    def local(w1, w2, x, dy):
        nl, nd, ff = w1.shape
        tok = x.shape[0] * x.shape[1] * x.shape[2]

        def mm(a, b):
            return jnp.dot(a, b, preferred_element_type=F32)

        h = x.reshape(tok, nd)
        g = dy.reshape(tok, nd)
        hs, us, acts = [], [], []
        for l in range(nl):
            u = mm(h, w1[l]).astype(BF16)
            act = gelu_pair(u.astype(F32))[0].astype(BF16)
            hs.append(h)
            us.append(u)
            acts.append(act)
            if l + 1 < nl:
                h = (h.astype(F32) + mm(act, w2[l])).astype(BF16)
        mine, o, dx = reduce_all(sizes, ff, nd, tok, [hs[0], g, hs[1], acts[1], acts[0], us[1], us[0], w1, w2])
        g1, g2 = place(mine, o, nl, ff, nd)
        return g1, g2, dx.reshape(x.shape)

    return jax.shard_map(local, mesh=mesh, in_specs=(P(), P(), P(AXES), P(AXES)), out_specs=(P(), P(), P(AXES)), check_vma=False)
```
